256 devices in a mesh: gx: 8 (over z), gy: 4 (over y), gz: 8 (over x, core).
Axes of the slice: x: 4, y: 4, z: 8, core: 2. Of those that a mesh axis runs over, the one named last changes fastest.
Arguments:
- signal: float32 [16, 1048576], P(None, ('gx', 'gy', 'gz')), may hold values from -6 to 6
- order: int32 [1048576], P(('gx', 'gy', 'gz')), may hold values from 0 to 4095, as said below
- near_tiles: bfloat16 [4096, 3, 256, 256], P(('gx', 'gy', 'gz')), may hold values from -0.21875 to 0.21875
- near_list: int32 [4096, 3], P(('gx', 'gy', 'gz')), may hold values from 0 to 4095, as said below
- leaf_basis: bfloat16 [4096, 64, 256], P(('gx', 'gy', 'gz')), may hold values from -0.375 to 0.375
- leaf_transfer: bfloat16 [4096, 64, 64], P(('gx', 'gy', 'gz')), may hold values from -0.5 to 0.5
- leaf_coupling: bfloat16 [4096, 64, 192], P(('gx', 'gy', 'gz')), may hold values from -0.4375 to 0.4375
- leaf_links: int32 [4096, 3], P(('gx', 'gy', 'gz')), may hold values from 0 to 4095, as said below
- device_transfer: bfloat16 [256, 64, 64], P(('gx', 'gy', 'gz')), may hold values from -0.5 to 0.5
- device_coupling: bfloat16 [256, 64, 192], P(('gx', 'gy', 'gz')), may hold values from -0.15625 to 0.15625
- device_links: int32 [256, 3], P(('gx', 'gy', 'gz')), may hold values from 0 to 255, as said below
- block_transfer: bfloat16 [32, 64, 64], P(('gx', 'gy')), may hold values from -0.5 to 0.5
- block_coupling: bfloat16 [32, 64, 192], P(('gx', 'gy')), may hold values from -0.078125 to 0.078125
- block_links: int32 [32, 3], P(('gx', 'gy')), may hold values from 0 to 31, as said below
- top_coupling: bfloat16 [8, 64, 192], P('gx'), may hold values from -0.0546875 to 0.0546875
- top_links: int32 [8, 3], P('gx'), may hold values from 0 to 7, as said below
Outputs:
- smoothed: float32 [16, 1048576], P(None, ('gx', 'gy', 'gz'))
- twice: float32 [16, 1048576], P(None, ('gx', 'gy', 'gz'))
The draws below stay inside these ranges and needn't reach their ends.
Inputs may be any that keep to these rules, and one draw needn't show every extreme that they name: `order`: each device's block of 4096 consecutive entries is a permutation of 0 to 4095. `near_list`: row i holds i first, then two different leaves j with 1 <= |j - i| <= 2. `leaf_links`: row i holds three different leaves j with 2 <= |j - i| <= 4. `device_links`: row i holds three different device clusters j with 1 <= |j - i| <= 3. `block_links`: row i holds three different second-level clusters other than i. `top_links`: row i holds three different first-level clusters other than i.
All inputs are finite; a program needn't handle non-finite values.
Results may differ from the reference program's by a relative error of at most 0.0043.
Values may be sent and summed in bfloat16 or wider, within the bound.
A program may use at most 64 MiB of HBM per device.

```python
import jax
import jax.numpy as jnp
from jax import lax

LEAF = 256
RANK = 64
RHS = 16
LEAF_DEV = 16
NEAR = 3
LINKS = 3
NEAR_REACH = 2
LINK_REACH = 4
DEVICE_REACH = 3
POINT_DEV = 4096
LEAVES = 4096
POINTS = 1048576
BLOCKS = 32
TOPS = 8
N_GY = 4
N_GZ = 8
DEVICES = 256


def pick_offsets(key, node_count, offsets, chosen):
    row_ids = jnp.arange(node_count, dtype=jnp.int32)[:, None]
    candidates = row_ids + offsets[None, :]
    usable = (candidates >= 0) & (candidates < node_count)
    span_count = offsets.shape[0]
    columns = jnp.arange(span_count, dtype=jnp.int32)[None, :]
    scores = jax.random.randint(key, (node_count, span_count), 0, 4096, dtype=jnp.int32) * span_count + columns
    scores = jnp.where(usable, scores, -1 - columns)
    ranked = jnp.argsort(-scores, axis=1)[:, :chosen]
    return jnp.take_along_axis(candidates, ranked, axis=1).astype(jnp.int32)


def pick_others(key, node_count, chosen):
    columns = jnp.arange(node_count, dtype=jnp.int32)[None, :]
    row_ids = jnp.arange(node_count, dtype=jnp.int32)[:, None]
    scores = jax.random.randint(key, (node_count, node_count), 0, 4096, dtype=jnp.int32) * node_count + columns
    scores = jnp.where(columns == row_ids, -1, scores)
    ranked = jnp.argsort(-scores, axis=1)[:, :chosen]
    return ranked.astype(jnp.int32)


def draw_order(key, part):
    block_count = POINTS // POINT_DEV
    keys_all = jax.random.split(jax.random.fold_in(key, 3), block_count)
    perms = jax.vmap(lambda single: jax.random.permutation(single, POINT_DEV))(keys_all)
    return perms.reshape(POINTS).astype(jnp.int32)


def draw_near_list(key, part):
    offsets = jnp.concatenate([jnp.arange(-NEAR_REACH, 0, dtype=jnp.int32), jnp.arange(1, NEAR_REACH + 1, dtype=jnp.int32)])
    others = pick_offsets(jax.random.fold_in(key, 5), LEAVES, offsets, NEAR - 1)
    itself = jnp.arange(LEAVES, dtype=jnp.int32)[:, None]
    return jnp.concatenate([itself, others], axis=1)


def draw_leaf_links(key, part):
    offsets = jnp.concatenate([jnp.arange(-LINK_REACH, -1, dtype=jnp.int32), jnp.arange(2, LINK_REACH + 1, dtype=jnp.int32)])
    return pick_offsets(jax.random.fold_in(key, 7), LEAVES, offsets, LINKS)


def draw_device_links(key, part):
    offsets = jnp.concatenate([jnp.arange(-DEVICE_REACH, 0, dtype=jnp.int32), jnp.arange(1, DEVICE_REACH + 1, dtype=jnp.int32)])
    return pick_offsets(jax.random.fold_in(key, 9), LEAVES // LEAF_DEV, offsets, LINKS)


def draw_block_links(key, part):
    return pick_others(jax.random.fold_in(key, 11), BLOCKS, LINKS)


def draw_top_links(key, part):
    return pick_others(jax.random.fold_in(key, 13), TOPS, LINKS)


def block_levels(own_key, extent, pieces, smallest, largest):
    gain, own = 1.0, jax.random.fold_in(own_key, 6)
    for position, blocks in pieces:
        steps = jnp.exp(jax.random.uniform(jax.random.fold_in(own, position), (blocks,), jnp.float32, smallest / len(pieces), largest / len(pieces)))
        gain = gain * jnp.repeat(steps, extent[position] // blocks).reshape([-1 if axis == position else 1 for axis in range(len(extent))])
    return gain


def gaussian(key, shape, deviation, bound, shards=(), kind=jnp.bfloat16):
    factor_of = block_levels(key, shape, shards, -0.22, 0.18) if shards else 1.0
    array = jax.random.normal(key, shape, jnp.float32) * deviation * factor_of
    return jnp.minimum(jnp.maximum(array, -bound), bound).astype(kind)


def setup_inputs(seed: int = 0) -> dict:
    key_of = jax.random.split(jax.random.key(seed), 17)
    signal = gaussian(key_of[0], (RHS, POINTS), 1.0, 6.0, ((1, 256),), jnp.float32)
    order = draw_order(jax.random.fold_in(key_of[16], 71), 0)
    near_tiles = gaussian(key_of[2], (LEAVES, NEAR, LEAF, LEAF), (NEAR * LEAF) ** -0.5, 0.21875, ((0, 256),))
    near_list = draw_near_list(jax.random.fold_in(key_of[16], 71), 0)
    leaf_basis = gaussian(key_of[4], (LEAVES, RANK, LEAF), LEAF ** -0.5, 0.375, ((0, 256),))
    leaf_transfer = gaussian(key_of[5], (LEAVES, RANK, RANK), (2 * RANK) ** -0.5, 0.5, ((0, 256),))
    leaf_coupling = gaussian(key_of[6], (LEAVES, RANK, LINKS * RANK), (RANK * LINKS) ** -0.5, 0.4375, ((0, 256),))
    leaf_links = draw_leaf_links(jax.random.fold_in(key_of[16], 71), 0)
    device_transfer = gaussian(key_of[8], (DEVICES, RANK, RANK), (2 * RANK) ** -0.5, 0.5, ((0, 256),))
    device_coupling = gaussian(key_of[9], (DEVICES, RANK, LINKS * RANK), (RANK * LINKS * LEAF_DEV // 2) ** -0.5, 0.15625, ((0, 256),))
    device_links = draw_device_links(jax.random.fold_in(key_of[16], 71), 0)
    block_transfer = gaussian(key_of[11], (BLOCKS, RANK, RANK), (2 * RANK) ** -0.5, 0.5, ((0, 32),))
    block_coupling = gaussian(key_of[12], (BLOCKS, RANK, LINKS * RANK), (RANK * LINKS * LEAF_DEV * N_GZ // 4) ** -0.5, 0.078125, ((0, 32),))
    block_links = draw_block_links(jax.random.fold_in(key_of[16], 71), 0)
    top_coupling = gaussian(key_of[14], (TOPS, RANK, LINKS * RANK), (RANK * LINKS * LEAF_DEV * N_GZ * N_GY // 8) ** -0.5, 0.0546875, ((0, 8),))
    top_links = draw_top_links(jax.random.fold_in(key_of[16], 71), 0)
    return {"signal": signal, "order": order, "near_tiles": near_tiles, "near_list": near_list, "leaf_basis": leaf_basis, "leaf_transfer": leaf_transfer, "leaf_coupling": leaf_coupling, "leaf_links": leaf_links, "device_transfer": device_transfer, "device_coupling": device_coupling, "device_links": device_links, "block_transfer": block_transfer, "block_coupling": block_coupling, "block_links": block_links, "top_coupling": top_coupling, "top_links": top_links}


HIGH = lax.Precision.HIGHEST


def couple_all(moments, links, coupling):
    node_count = coupling.shape[0]
    table = coupling.astype(jnp.float32).reshape(node_count, RANK, LINKS, RANK)
    return jnp.einsum('rnjk,nkjm->rnm', moments[:, links], table, precision=HIGH)


def gather_up(child, transfer, group):
    shaped = child.reshape(RHS, -1, group, RANK)
    weights = transfer.astype(jnp.float32).reshape(-1, group, RANK, RANK)
    return jnp.einsum('rngk,ngkm->rnm', shaped, weights, precision=HIGH)


def spread(parent, transfer, group):
    repeated = jnp.repeat(parent, group, axis=1)
    return jnp.einsum('rnm,nkm->rnk', repeated, transfer.astype(jnp.float32), precision=HIGH)


def near_field(leaves, near_tiles, near_list):
    device_count = LEAVES // LEAF_DEV

    def one_block(inputs):
        tiles, lists = inputs
        near_rows = leaves[:, lists].astype(jnp.float32)
        return jnp.einsum('rlns,lnst->rlt', near_rows, tiles.astype(jnp.float32))

    blocks = lax.map(one_block, (near_tiles.reshape(device_count, LEAF_DEV, NEAR, LEAF, LEAF), near_list.reshape(device_count, LEAF_DEV, NEAR)))
    return jnp.transpose(blocks, (1, 0, 2, 3)).reshape(RHS, LEAVES, LEAF)


def apply_matrix(leaves, near_tiles, near_list, leaf_basis, leaf_transfer, leaf_coupling, leaf_links, device_transfer, device_coupling, device_links, block_transfer, block_coupling, block_links, top_coupling, top_links):
    basis_f = leaf_basis.astype(jnp.float32)
    moments = jnp.einsum('rls,lks->rlk', leaves.astype(jnp.float32), basis_f)
    device_moment = gather_up(moments, leaf_transfer, LEAF_DEV)
    block_moment = gather_up(device_moment, device_transfer, N_GZ)
    top_moment = gather_up(block_moment, block_transfer, N_GY)
    top_field = couple_all(top_moment, top_links, top_coupling)
    block_field = couple_all(block_moment, block_links, block_coupling) + spread(top_field, block_transfer, N_GY)
    device_field = couple_all(device_moment, device_links, device_coupling) + spread(block_field, device_transfer, N_GZ)
    leaf_field = couple_all(moments, leaf_links, leaf_coupling) + spread(device_field, leaf_transfer, LEAF_DEV)
    rounded = leaf_field.astype(jnp.bfloat16).astype(jnp.float32)
    far_part = jnp.einsum('rlk,lks->rls', rounded, basis_f)
    return near_field(leaves, near_tiles, near_list) + far_part


def reference(signal, order, near_tiles, near_list, leaf_basis, leaf_transfer, leaf_coupling, leaf_links, device_transfer, device_coupling, device_links, block_transfer, block_coupling, block_links, top_coupling, top_links):
    positions = (jnp.arange(POINTS, dtype=jnp.int32) // POINT_DEV) * POINT_DEV + order.astype(jnp.int32)
    matrices = (near_tiles, near_list, leaf_basis, leaf_transfer, leaf_coupling, leaf_links, device_transfer, device_coupling, device_links, block_transfer, block_coupling, block_links, top_coupling, top_links)
    tree = signal[:, positions].astype(jnp.bfloat16).reshape(RHS, LEAVES, LEAF)
    first = apply_matrix(tree, *matrices)
    second = apply_matrix(first.astype(jnp.bfloat16), *matrices)
    empty = jnp.zeros((RHS, POINTS), jnp.float32)
    smoothed = empty.at[:, positions].set(first.reshape(RHS, POINTS))
    twice = empty.at[:, positions].set(second.reshape(RHS, POINTS))
    return smoothed, twice
```

```python
import functools

import jax
import jax.numpy as jnp
from jax import lax
from jax.experimental import pallas as pl
from jax.experimental.pallas import tpu as pltpu
from jax.sharding import PartitionSpec as P

MESH = pl.DeviceIdType.MESH
NEAR_REACH = 2
LINK_REACH = 4
DEVICE_REACH = 3
LINKS = 3
F32 = jnp.float32
BF16 = jnp.bfloat16


def nn(a, b):
    return lax.dot_general(a, b, (((1,), (0,)), ((), ())), preferred_element_type=F32)


def nt(a, b):
    return lax.dot_general(a, b, (((1,), (1,)), ((), ())), preferred_element_type=F32)


def within(index, ref):
    return jnp.minimum(jnp.maximum(index, 0), ref.shape[0] - 1)


def halves(x):
    top = x.astype(BF16)
    return jnp.concatenate([top, (x - top.astype(F32)).astype(BF16)], axis=0)


def fine(product, x, weights):
    both = product(halves(x), weights)
    return both[: x.shape[0]] + both[x.shape[0] :]


def parts_of(x):
    top = x.astype(BF16)
    return top, (x - top.astype(F32)).astype(BF16)


def full(x, tops, rests):
    both = nn(halves(x), tops)
    return both[: x.shape[0]] + both[x.shape[0] :] + nn(x.astype(BF16), rests)


def placed(rows, cols, offset):
    i = lax.broadcasted_iota(jnp.int32, (rows, cols), 0)
    j = lax.broadcasted_iota(jnp.int32, (rows, cols), 1)
    return jnp.where(j == i + offset, 1.0, 0.0).astype(F32)


def kernel(
    n_gx,
    n_gy,
    n_gz,
    near_list,
    leaf_links,
    device_links,
    block_links,
    top_links,
    signal,
    order,
    near_tiles,
    leaf_basis,
    leaf_transfer,
    leaf_coupling,
    device_transfer,
    device_coupling,
    block_transfer,
    block_coupling,
    top_coupling,
    smoothed,
    twice,
    sig_v,
    ord_v,
    tiles_v,
    basis_v,
    lt_v,
    lc_v,
    dt_v,
    dc_v,
    bt_v,
    bc_v,
    tc_v,
    hot_v,
    scat_v,
    vw_0,
    vw_1,
    mw_0,
    mw_1,
    raw_0,
    raw_1,
    r1_src,
    r1_buf,
    r2_0,
    r2_1,
    near_v,
    coup_v,
    qt_v,
    mix_v,
    local_sem,
    halo_send,
    halo_recv,
    raw_send,
    raw_recv,
    r1_send,
    r1_recv,
    r2_send,
    r2_recv,
):
    rhs, points = sig_v.shape
    leaves, rank, leaf = basis_v.shape
    slabs = points // leaf
    n_blocks = n_gx * n_gy
    n_devices = n_blocks * n_gz
    gx, gy, gz = lax.axis_index("gx"), lax.axis_index("gy"), lax.axis_index("gz")
    block = gx * n_gy + gy
    device = block * n_gz + gz
    first_leaf = device * leaves

    def mesh_id(index):
        index = lax.rem(index + n_devices, n_devices)
        row = index // n_gz
        return {"gx": row // n_gy, "gy": lax.rem(row, n_gy), "gz": lax.rem(index, n_gz)}

    def plane_id(k):
        other = lax.rem(block + k, n_blocks)
        return {"gx": other // n_gy, "gy": lax.rem(other, n_gy), "gz": gz}

    def line_id(k):
        return {"gx": gx, "gy": gy, "gz": lax.rem(gz + k, n_gz)}

    sides = (-3, -2, -1, 1, 2, 3)
    vw, mw, raw_v, r2_buf = (vw_0, vw_1), (mw_0, mw_1), (raw_0, raw_1), (r2_0, r2_1)

    def load(src, dst, slot):
        copy = pltpu.make_async_copy(src, dst, local_sem.at[slot])
        copy.start()
        return copy

    c_order = load(order, ord_v, 0)
    c_signal = load(signal, sig_v, 1)
    c_dt = load(device_transfer, dt_v, 2)
    c_bt = load(block_transfer, bt_v, 3)
    c_basis = load(leaf_basis, basis_v, 4)
    c_lt = load(leaf_transfer, lt_v, 5)
    c_dc = load(device_coupling, dc_v, 6)
    c_bc = load(block_coupling, bc_v, 7)
    c_tc = load(top_coupling, tc_v, 8)
    c_tiles = load(near_tiles, tiles_v, 9)
    c_lc = load(leaf_coupling, lc_v, 10)

    barrier = pltpu.get_barrier_semaphore()

    @pl.loop(1, n_gz)
    def _(k):
        pl.semaphore_signal(barrier, inc=1, device_id=line_id(k), device_id_type=MESH)

    @pl.loop(1, n_blocks)
    def _(k):
        pl.semaphore_signal(barrier, inc=1, device_id=plane_id(k), device_id_type=MESH)

    for s in sides:
        pl.semaphore_signal(
            barrier, inc=1, device_id=mesh_id(device + s), device_id_type=MESH
        )

    c_dt.wait()
    c_bt.wait()
    own_dt = dt_v[0]
    own_bt = bt_v[0]
    up = placed(rank, 4 * rank, 0) + nn(own_bt, placed(rank, 4 * rank, rank).astype(BF16))
    e1 = parts_of(nn(own_dt, up.astype(BF16)) + placed(rank, 4 * rank, 3 * rank))

    c_order.wait()
    c_signal.wait()
    sig_rows = jnp.concatenate(
        [sig_v[:, q * leaf : (q + 1) * leaf].astype(BF16) for q in range(slabs)], axis=0
    )
    lane_rows = lax.broadcasted_iota(jnp.int32, (leaf, leaf), 0)
    c_basis.wait()
    c_lt.wait()

    upper_lanes = lax.broadcasted_iota(jnp.int32, (rhs, 2 * rank), 1) >= rank

    def twofold(x):
        return jnp.concatenate([x, x], axis=0)

    def moments_of(value, l):
        both = nt(value, twofold(basis_v[l]))
        top = both.astype(BF16).astype(F32)
        return jnp.where(upper_lanes, both - top, top).astype(BF16)

    own = jnp.zeros((rhs, rank), F32)
    for j in range(leaves):
        cols = slice(j * leaf, (j + 1) * leaf)
        spot = ord_v[:, cols]
        low = lax.rem(spot, leaf)
        high = spot // leaf
        hot = jnp.where(lane_rows == low, 1.0, 0.0).astype(BF16)
        hot_v[:, cols] = hot
        picked = nn(sig_rows, hot)
        value = jnp.zeros((rhs, leaf), F32)
        for q in range(slabs):
            value = value + jnp.where(high == q, picked[q * rhs : (q + 1) * rhs], 0.0)
        value = value.astype(BF16)
        vw[0][NEAR_REACH + j] = value
        moment = moments_of(value, j)
        mw[0][LINK_REACH + j] = moment
        own = own + nn(moment, twofold(lt_v[j]))
    msg = full(own, *e1)

    pl.semaphore_wait(barrier, (n_gz - 1) + (n_blocks - 1) + len(sides))

    def r1_copy(a, k):
        return pltpu.make_async_remote_copy(
            src_ref=r1_src.at[a],
            dst_ref=r1_buf.at[a, k],
            send_sem=r1_send.at[a, k],
            recv_sem=r1_recv.at[a, k],
            device_id=line_id(k),
            device_id_type=MESH,
        )

    def r2_copy(a, k):
        return pltpu.make_async_remote_copy(
            src_ref=r2_buf[a].at[block],
            dst_ref=r2_buf[a].at[block],
            send_sem=r2_send.at[a, k],
            recv_sem=r2_recv.at[a, k],
            device_id=plane_id(k),
            device_id_type=MESH,
        )

    def raw_copy(a, n):
        s = sides[n]
        return pltpu.make_async_remote_copy(
            src_ref=raw_v[a].at[DEVICE_REACH],
            dst_ref=raw_v[a].at[DEVICE_REACH - s],
            send_sem=raw_send.at[a, n],
            recv_sem=raw_recv.at[a, n],
            device_id=mesh_id(device + s),
            device_id_type=MESH,
        )

    def halo_copy(a, n):
        ref, reach = (vw, NEAR_REACH) if n < 2 else (mw, LINK_REACH)
        if n % 2 == 0:
            src, dst, s = leaves, 0, 1
        else:
            src, dst, s = reach, reach + leaves, -1
        return pltpu.make_async_remote_copy(
            src_ref=ref[a].at[pl.ds(src, reach)],
            dst_ref=ref[a].at[pl.ds(dst, reach)],
            send_sem=halo_send.at[a, n],
            recv_sem=halo_recv.at[a, n],
            device_id=mesh_id(device + s),
            device_id_type=MESH,
        )

    def send_up(a, message):
        r1_src[a] = message[:, 0 : 2 * rank].astype(BF16)
        raw_v[a][DEVICE_REACH] = message[:, 2 * rank : 4 * rank]

        @pl.loop(1, n_gz)
        def _(k):
            r1_copy(a, k).start()

        for n in range(len(sides)):
            raw_copy(a, n).start()

    def send_across(a):
        @pl.loop(1, n_gz)
        def _(k):
            r1_copy(a, k).wait_recv()

        total = r1_src[a].astype(F32)
        for k in range(1, n_gz):
            total = total + r1_buf[a, k].astype(F32)
        r2_buf[a][block] = total.astype(BF16)

        @pl.loop(1, n_blocks)
        def _(k):
            r2_copy(a, k).start()

    def wait_across(a):
        @pl.loop(1, n_blocks)
        def _(k):
            r2_copy(a, k).wait_recv()

    def far_part(a):
        parts = [r2_buf[a][block_links[0, k]].astype(BF16) for k in range(LINKS)]
        for k in range(LINKS):
            total = jnp.zeros((rhs, 2 * rank), F32)
            for i in range(n_gy):
                total = total + r2_buf[a][top_links[0, k] * n_gy + i].astype(F32)
            parts.append(total.astype(BF16))
        rows = jnp.concatenate(parts, axis=1)
        start = LINKS * 2 * rank
        return nn(rows, mix_v[0, start:]) + nn(rows, mix_v[1, start:])

    def side_part(a):
        for n in range(len(sides)):
            raw_copy(a, n).wait_recv()
        parts = [
            raw_v[a][within(device_links[0, k] - device + DEVICE_REACH, raw_v[a])]
            for k in range(LINKS)
        ]
        end = LINKS * 2 * rank
        return full(jnp.concatenate(parts, axis=1), mix_v[0, :end], mix_v[1, :end])

    def field_of(message):
        field = message[:, 2 * rank : 3 * rank]
        return halves(jnp.concatenate([field, field], axis=1))

    def twice_rows(both):
        return both[0:rhs] + both[rhs:]

    def send_halos(a):
        for n in range(4):
            halo_copy(a, n).start()

    def wait_halos(a):
        for n in range(4):
            halo_copy(a, n).wait_recv()

    def near_and_leaf(a):
        diagonal = lax.broadcasted_iota(jnp.int32, (rhs, LINKS * rank), 1) // rank
        for l in range(leaves):
            total = nn(vw[a][NEAR_REACH + l], tiles_v[l, 0])
            for k in range(1, near_list.shape[0]):
                spot = within(near_list[k, l] - first_leaf + NEAR_REACH, vw[a])
                total = total + nn(vw[a][spot], tiles_v[l, k])
            near_v[l] = total
            stacked = jnp.concatenate(
                [
                    mw[a][within(leaf_links[k, l] - first_leaf + LINK_REACH, mw[a])]
                    for k in range(LINKS)
                ],
                axis=0,
            )
            wide = nn(stacked, twofold(lc_v[l]))
            kept = wide[0:rhs]
            for k in range(1, LINKS):
                kept = jnp.where(diagonal == k, wide[k * rhs : (k + 1) * rhs], kept)
            coup_v[l * 2 * rhs : (l + 1) * 2 * rhs, :] = halves(kept)
        fold = placed(LINKS * rank, rank, 0)
        for k in range(1, LINKS):
            fold = fold + placed(LINKS * rank, rank, -k * rank)
        field = nn(coup_v[...], fold.astype(BF16))
        for l in range(leaves):
            base = l * 2 * rhs
            whole = field[base : base + rhs] + field[base + rhs : base + 2 * rhs]
            near_v[l] = near_v[l] + fine(nn, whole, basis_v[l])

    def scatter(target):
        for j in range(leaves):
            cols = slice(j * leaf, (j + 1) * leaf)
            value = near_v[j]
            top = value.astype(BF16).astype(F32)
            rest = value - top
            high = ord_v[:, cols] // leaf
            for q in range(slabs):
                here = high == q
                rows = slice(q * rhs, (q + 1) * rhs)
                scat_v[rows, cols] = jnp.where(here, top, 0.0).astype(BF16)
                rows = slice((slabs + q) * rhs, (slabs + q + 1) * rhs)
                scat_v[rows, cols] = jnp.where(here, rest, 0.0).astype(BF16)
        done = nt(scat_v[...], hot_v[...])
        done = done[: slabs * rhs] + done[slabs * rhs :]
        for q in range(slabs):
            target[:, q * leaf : (q + 1) * leaf] = done[q * rhs : (q + 1) * rhs]

    send_up(0, msg)
    send_halos(0)

    c_dc.wait()
    c_bc.wait()
    c_tc.wait()
    eye = placed(rank, rank, 0).astype(BF16)
    square = jnp.zeros((rank, rank), F32)
    for l in range(leaves):
        turned = nt(eye, lt_v[l]).astype(BF16)
        qt = halves(nn(turned, basis_v[l]))
        qt_v[l] = qt
        square = square + nt(qt[0:rank], qt[0:rank])
    e2 = parts_of(full(square, *e1) + placed(rank, 4 * rank, 2 * rank))
    picks = [placed(LINKS * rank, rank, -k * rank).astype(BF16) for k in range(LINKS)]
    sides_in = [nn(dc_v[0], pick) for pick in picks]
    blocks_in = [nt(nn(bc_v[0], pick).astype(BF16), own_dt) for pick in picks]
    tops_in = [
        fine(nt, nt(nn(tc_v[0], pick).astype(BF16), own_bt), own_dt) for pick in picks
    ]
    mixed = full(jnp.concatenate(sides_in + blocks_in + tops_in, axis=0), *e2)
    mix_v[...] = jnp.zeros_like(mix_v)
    for n in range(3 * LINKS):
        base = n * 2 * rank + (0 if LINKS <= n < 2 * LINKS else rank)
        for half, value in enumerate(parts_of(mixed[n * rank : (n + 1) * rank])):
            mix_v[half, base : base + rank, :] = value

    send_across(0)

    c_tiles.wait()
    c_lc.wait()
    wait_halos(0)
    near_and_leaf(0)
    local = jnp.zeros((rhs, rank), F32)
    for l in range(leaves):
        local = local + nt(near_v[l].astype(BF16), qt_v[l, 0:rank])
    partial = full(local, *e1) + side_part(0)

    wait_across(0)
    msg = partial + far_part(0)
    send_up(1, msg)

    field = field_of(msg)
    for l in range(leaves):
        value = near_v[l] + twice_rows(nn(field, qt_v[l]))
        near_v[l] = value
        value = value.astype(BF16)
        vw[1][NEAR_REACH + l] = value
        mw[1][LINK_REACH + l] = moments_of(value, l)
    send_halos(1)
    scatter(smoothed)
    send_across(1)
    wait_halos(1)
    near_and_leaf(1)
    partial = side_part(1)
    wait_across(1)
    msg = partial + far_part(1)
    field = field_of(msg)
    for l in range(leaves):
        near_v[l] = near_v[l] + twice_rows(nn(field, qt_v[l]))
    scatter(twice)

    for a in range(2):

        @pl.loop(1, n_gz)
        def _(k):
            r1_copy(a, k).wait_send()

        @pl.loop(1, n_blocks)
        def _(k):
            r2_copy(a, k).wait_send()

        for n in range(len(sides)):
            raw_copy(a, n).wait_send()
        for n in range(4):
            halo_copy(a, n).wait_send()


def solution(mesh):
    sizes = mesh.shape["gx"], mesh.shape["gy"], mesh.shape["gz"]
    n_gx, n_gy, n_gz = sizes

    def shards(
        signal,
        order,
        near_tiles,
        near_list,
        leaf_basis,
        leaf_transfer,
        leaf_coupling,
        leaf_links,
        device_transfer,
        device_coupling,
        device_links,
        block_transfer,
        block_coupling,
        block_links,
        top_coupling,
        top_links,
    ):
        rhs, points = signal.shape
        leaves, rank, leaf = leaf_basis.shape
        n_blocks = n_gx * n_gy
        vmem, far = pltpu.VMEM, pl.BlockSpec(memory_space=pltpu.HBM)
        smem = pl.BlockSpec(memory_space=pltpu.SMEM)
        wide = 2 * rank
        dma = pltpu.SemaphoreType.DMA
        scratch = [
            vmem((rhs, points), F32),
            vmem((1, points), jnp.int32),
            vmem(near_tiles.shape, BF16),
            vmem(leaf_basis.shape, BF16),
            vmem(leaf_transfer.shape, BF16),
            vmem(leaf_coupling.shape, BF16),
            vmem(device_transfer.shape, BF16),
            vmem(device_coupling.shape, BF16),
            vmem(block_transfer.shape, BF16),
            vmem(block_coupling.shape, BF16),
            vmem(top_coupling.shape, BF16),
            vmem((leaf, points), BF16),
            vmem((2 * rhs * points // leaf, points), BF16),
            vmem((leaves + 2 * NEAR_REACH, rhs, leaf), BF16),
            vmem((leaves + 2 * NEAR_REACH, rhs, leaf), BF16),
            vmem((leaves + 2 * LINK_REACH, rhs, wide), BF16),
            vmem((leaves + 2 * LINK_REACH, rhs, wide), BF16),
            vmem((2 * DEVICE_REACH + 1, rhs, wide), F32),
            vmem((2 * DEVICE_REACH + 1, rhs, wide), F32),
            vmem((2, rhs, wide), BF16),
            vmem((2, n_gz, rhs, wide), BF16),
            vmem((n_blocks, rhs, wide), BF16),
            vmem((n_blocks, rhs, wide), BF16),
            vmem((leaves, rhs, leaf), F32),
            vmem((2 * leaves * rhs, LINKS * rank), BF16),
            vmem((leaves, 2 * rank, leaf), BF16),
            vmem((2, 3 * LINKS * wide, 4 * rank), BF16),
            dma((11,)),
            dma((2, 4)),
            dma((2, 4)),
            dma((2, 6)),
            dma((2, 6)),
            dma((2, n_gz)),
            dma((2, n_gz)),
            dma((2, n_blocks)),
            dma((2, n_blocks)),
        ]
        out = jax.ShapeDtypeStruct((rhs, points), F32)
        return pl.pallas_call(
            functools.partial(kernel, n_gx, n_gy, n_gz),
            out_shape=(out, out),
            in_specs=[smem] * 5 + [far] * 11,
            out_specs=(pl.BlockSpec(memory_space=vmem),) * 2,
            scratch_shapes=scratch,
            compiler_params=pltpu.CompilerParams(
                collective_id=0, has_side_effects=True, vmem_limit_bytes=60 * 1024 * 1024
            ),
        )(
            near_list.T,
            leaf_links.T,
            device_links,
            block_links,
            top_links,
            signal,
            order.reshape(1, points),
            near_tiles,
            leaf_basis,
            leaf_transfer,
            leaf_coupling,
            device_transfer,
            device_coupling,
            block_transfer,
            block_coupling,
            top_coupling,
        )

    every = ("gx", "gy", "gz")
    in_specs = (
        P(None, every),
        P(every),
        P(every, None, None, None),
        P(every, None),
        P(every, None, None),
        P(every, None, None),
        P(every, None, None),
        P(every, None),
        P(every, None, None),
        P(every, None, None),
        P(every, None),
        P(("gx", "gy"), None, None),
        P(("gx", "gy"), None, None),
        P(("gx", "gy"), None),
        P("gx", None, None),
        P("gx", None),
    )
    out_specs = (P(None, every), P(None, every))
    return jax.shard_map(
        shards, mesh=mesh, in_specs=in_specs, out_specs=out_specs, check_vma=False
    )
```

```python
import functools

import jax
import jax.numpy as jnp
from jax import lax
from jax.experimental import pallas as pl
from jax.experimental.pallas import tpu as pltpu
from jax.sharding import PartitionSpec as P

MESH = pl.DeviceIdType.MESH
NEAR_REACH = 2
LINK_REACH = 4
DEVICE_REACH = 3
LINKS = 3
F32 = jnp.float32
BF16 = jnp.bfloat16


def nn(a, b):
    return lax.dot_general(a, b, (((1,), (0,)), ((), ())), preferred_element_type=F32)


def nt(a, b):
    return lax.dot_general(a, b, (((1,), (1,)), ((), ())), preferred_element_type=F32)


def within(index, ref):
    return jnp.minimum(jnp.maximum(index, 0), ref.shape[0] - 1)


def halves(x):
    top = x.astype(BF16)
    return jnp.concatenate([top, (x - top.astype(F32)).astype(BF16)], axis=0)


def fine(product, x, weights):
    both = product(halves(x), weights)
    return both[: x.shape[0]] + both[x.shape[0] :]


def parts_of(x):
    top = x.astype(BF16)
    return top, (x - top.astype(F32)).astype(BF16)


def full(x, tops, rests):
    both = nn(halves(x), tops)
    return both[: x.shape[0]] + both[x.shape[0] :] + nn(x.astype(BF16), rests)


def placed(rows, cols, offset):
    i = lax.broadcasted_iota(jnp.int32, (rows, cols), 0)
    j = lax.broadcasted_iota(jnp.int32, (rows, cols), 1)
    return jnp.where(j == i + offset, 1.0, 0.0).astype(F32)


def kernel(
    n_gx,
    n_gy,
    n_gz,
    near_list,
    leaf_links,
    device_links,
    block_links,
    top_links,
    signal,
    order,
    near_tiles,
    leaf_basis,
    leaf_transfer,
    leaf_coupling,
    device_transfer,
    device_coupling,
    block_transfer,
    block_coupling,
    top_coupling,
    smoothed,
    twice,
    sig_v,
    ord_v,
    tiles_v,
    basis_v,
    lt_v,
    lc_v,
    dt_v,
    dc_v,
    bt_v,
    bc_v,
    tc_v,
    hot_v,
    scat_v,
    vw_0,
    vw_1,
    mw_0,
    mw_1,
    raw_0,
    raw_1,
    r1_src,
    r1_buf,
    r2_0,
    r2_1,
    near_v,
    coup_v,
    qt_v,
    mix_v,
    out_v,
    local_sem,
    out_sem,
    halo_send,
    halo_recv,
    raw_send,
    raw_recv,
    r1_send,
    r1_recv,
    r2_send,
    r2_recv,
):
    rhs, points = sig_v.shape
    leaves, rank, leaf = basis_v.shape
    slabs = points // leaf
    shift = leaf.bit_length() - 1
    assert 1 << shift == leaf
    n_blocks = n_gx * n_gy
    n_devices = n_blocks * n_gz
    gx, gy, gz = lax.axis_index("gx"), lax.axis_index("gy"), lax.axis_index("gz")
    block = gx * n_gy + gy
    device = block * n_gz + gz
    first_leaf = device * leaves

    def wrapped(index, size):
        index = jnp.where(index >= size, index - size, index)
        return jnp.where(index < 0, index + size, index)

    def mesh_id(shift):
        z = gz + shift
        carry = (z >= n_gz).astype(jnp.int32) - (z < 0).astype(jnp.int32)
        y = gy + carry
        carry = (y >= n_gy).astype(jnp.int32) - (y < 0).astype(jnp.int32)
        return {
            "gx": wrapped(gx + carry, n_gx),
            "gy": wrapped(y, n_gy),
            "gz": wrapped(z, n_gz),
        }

    def far_first(size):
        return sorted(range(size), key=lambda step: -min(step, size - step))

    plane = [(x, y) for x in far_first(n_gx) for y in far_first(n_gy) if x or y]

    def plane_id(k):
        x, y = plane[k]
        return {"gx": wrapped(gx + x, n_gx), "gy": wrapped(gy + y, n_gy), "gz": gz}

    line = [step for step in far_first(n_gz) if step]

    def line_id(k):
        return {"gx": gx, "gy": gy, "gz": wrapped(gz + line[k], n_gz)}

    sides = (-3, -2, -1, 1, 2, 3)
    vw, mw, raw_v, r2_buf = (vw_0, vw_1), (mw_0, mw_1), (raw_0, raw_1), (r2_0, r2_1)

    def load(src, dst, slot):
        copy = pltpu.make_async_copy(src, dst, local_sem.at[slot])
        copy.start()
        return copy

    c_order = load(order, ord_v, 0)
    c_signal = load(signal, sig_v, 1)
    c_dt = load(device_transfer, dt_v, 2)
    c_bt = load(block_transfer, bt_v, 3)
    c_basis = load(leaf_basis, basis_v, 4)
    c_lt = load(leaf_transfer, lt_v, 5)
    c_dc = load(device_coupling, dc_v, 6)
    c_bc = load(block_coupling, bc_v, 7)
    c_tc = load(top_coupling, tc_v, 8)
    c_tiles = load(near_tiles, tiles_v, 9)
    c_lc = load(leaf_coupling, lc_v, 10)

    barrier = pltpu.get_barrier_semaphore()

    peers = [plane_id(k) for k in range(len(plane))]
    peers = peers + [line_id(k) for k in range(len(line))] + [mesh_id(s) for s in sides]
    for peer in peers:
        pl.semaphore_signal(barrier, inc=1, device_id=peer, device_id_type=MESH)

    c_dt.wait()
    c_bt.wait()
    own_dt = dt_v[0]
    own_bt = bt_v[0]
    up = placed(rank, 4 * rank, 0) + nn(own_bt, placed(rank, 4 * rank, rank).astype(BF16))
    e1 = parts_of(nn(own_dt, up.astype(BF16)) + placed(rank, 4 * rank, 3 * rank))

    c_order.wait()
    c_signal.wait()
    sig_rows = jnp.concatenate(
        [sig_v[:, q * leaf : (q + 1) * leaf].astype(BF16) for q in range(slabs)], axis=0
    )
    def narrow(x):
        return x.astype(F32).astype(BF16)

    one, zero = jnp.ones((), BF16), jnp.zeros((), BF16)
    lane_rows = narrow(lax.broadcasted_iota(jnp.int32, (leaf, leaf), 0))
    c_basis.wait()
    c_lt.wait()

    upper_lanes = lax.broadcasted_iota(jnp.int32, (rhs, 2 * rank), 1) >= rank

    def twofold(x):
        return jnp.concatenate([x, x], axis=0)

    def moments_of(value, l):
        both = nt(value, twofold(basis_v[l]))
        top = both.astype(BF16).astype(F32)
        return jnp.where(upper_lanes, both - top, top).astype(BF16)

    own = jnp.zeros((rhs, rank), F32)
    for j in range(leaves):
        cols = slice(j * leaf, (j + 1) * leaf)
        spot = ord_v[:, cols]
        low = spot & (leaf - 1)
        high = lax.shift_right_logical(spot, shift)
        hot = jnp.where(lane_rows == narrow(low), one, zero)
        hot_v[:, cols] = hot
        picked = nn(sig_rows, hot)
        value = jnp.zeros((rhs, leaf), F32)
        for q in range(slabs):
            value = value + jnp.where(high == q, picked[q * rhs : (q + 1) * rhs], 0.0)
        value = value.astype(BF16)
        vw[0][NEAR_REACH + j] = value
        moment = moments_of(value, j)
        mw[0][LINK_REACH + j] = moment
        own = own + nn(moment, twofold(lt_v[j]))
    msg = full(own, *e1)

    pl.semaphore_wait(barrier, len(peers))

    def r1_copy(a, k):
        return pltpu.make_async_remote_copy(
            src_ref=r1_src.at[a],
            dst_ref=r1_buf.at[a, k],
            send_sem=r1_send.at[a, k],
            recv_sem=r1_recv.at[a, k],
            device_id=line_id(k),
            device_id_type=MESH,
        )

    def r2_copy(a, k):
        return pltpu.make_async_remote_copy(
            src_ref=r2_buf[a].at[block],
            dst_ref=r2_buf[a].at[block],
            send_sem=r2_send.at[a, k],
            recv_sem=r2_recv.at[a, k],
            device_id=plane_id(k),
            device_id_type=MESH,
        )

    def raw_copy(a, n):
        s = sides[n]
        return pltpu.make_async_remote_copy(
            src_ref=raw_v[a].at[DEVICE_REACH],
            dst_ref=raw_v[a].at[DEVICE_REACH - s],
            send_sem=raw_send.at[a, n],
            recv_sem=raw_recv.at[a, n],
            device_id=mesh_id(s),
            device_id_type=MESH,
        )

    def halo_copy(a, n):
        ref, reach = (vw, NEAR_REACH) if n < 2 else (mw, LINK_REACH)
        if n % 2 == 0:
            src, dst, s = leaves, 0, 1
        else:
            src, dst, s = reach, reach + leaves, -1
        return pltpu.make_async_remote_copy(
            src_ref=ref[a].at[pl.ds(src, reach)],
            dst_ref=ref[a].at[pl.ds(dst, reach)],
            send_sem=halo_send.at[a, n],
            recv_sem=halo_recv.at[a, n],
            device_id=mesh_id(s),
            device_id_type=MESH,
        )

    def send_up(a, message):
        r1_src[a] = message[:, 0 : 2 * rank].astype(BF16)
        raw_v[a][DEVICE_REACH] = message[:, 2 * rank : 4 * rank]

        for k in range(len(line)):
            r1_copy(a, k).start()
        for n in range(len(sides)):
            raw_copy(a, n).start()

    def send_across(a):
        for k in range(len(line)):
            r1_copy(a, k).wait_recv()
        total = r1_src[a].astype(F32)
        for k in range(len(line)):
            total = total + r1_buf[a, k].astype(F32)
        r2_buf[a][block] = total.astype(BF16)
        for k in range(len(plane)):
            r2_copy(a, k).start()

    def wait_across(a):
        for k in range(len(plane)):
            r2_copy(a, k).wait_recv()

    def far_part(a):
        parts = [r2_buf[a][block_links[0, k]].astype(BF16) for k in range(LINKS)]
        for k in range(LINKS):
            total = jnp.zeros((rhs, 2 * rank), F32)
            for i in range(n_gy):
                total = total + r2_buf[a][top_links[0, k] * n_gy + i].astype(F32)
            parts.append(total.astype(BF16))
        rows = jnp.concatenate(parts, axis=1)
        start = LINKS * 2 * rank
        return nn(rows, mix_v[0, start:]) + nn(rows, mix_v[1, start:])

    def side_part(a):
        for n in range(len(sides)):
            raw_copy(a, n).wait_recv()
        parts = [
            raw_v[a][within(device_links[0, k] - device + DEVICE_REACH, raw_v[a])]
            for k in range(LINKS)
        ]
        end = LINKS * 2 * rank
        return full(jnp.concatenate(parts, axis=1), mix_v[0, :end], mix_v[1, :end])

    def field_of(message):
        field = message[:, 2 * rank : 3 * rank]
        return halves(jnp.concatenate([field, field], axis=1))

    def twice_rows(both):
        return both[0:rhs] + both[rhs:]

    def send_halos(a):
        for n in range(4):
            halo_copy(a, n).start()

    def wait_halos(a):
        for n in range(4):
            halo_copy(a, n).wait_recv()

    def near_and_leaf(a):
        diagonal = lax.broadcasted_iota(jnp.int32, (rhs, LINKS * rank), 1) // rank
        for l in range(leaves):
            total = nn(vw[a][NEAR_REACH + l], tiles_v[l, 0])
            for k in range(1, near_list.shape[0]):
                spot = within(near_list[k, l] - first_leaf + NEAR_REACH, vw[a])
                total = total + nn(vw[a][spot], tiles_v[l, k])
            near_v[l] = total
            stacked = jnp.concatenate(
                [
                    mw[a][within(leaf_links[k, l] - first_leaf + LINK_REACH, mw[a])]
                    for k in range(LINKS)
                ],
                axis=0,
            )
            wide = nn(stacked, twofold(lc_v[l]))
            kept = wide[0:rhs]
            for k in range(1, LINKS):
                kept = jnp.where(diagonal == k, wide[k * rhs : (k + 1) * rhs], kept)
            coup_v[l * 2 * rhs : (l + 1) * 2 * rhs, :] = halves(kept)
        fold = placed(LINKS * rank, rank, 0)
        for k in range(1, LINKS):
            fold = fold + placed(LINKS * rank, rank, -k * rank)
        field = nn(coup_v[...], fold.astype(BF16))
        for l in range(leaves):
            base = l * 2 * rhs
            whole = field[base : base + rhs] + field[base + rhs : base + 2 * rhs]
            near_v[l] = near_v[l] + fine(nn, whole, basis_v[l])

    def scatter(target, slot):
        for j in range(leaves):
            cols = slice(j * leaf, (j + 1) * leaf)
            high = narrow(lax.shift_right_logical(ord_v[:, cols], shift))
            value = near_v[j].astype(BF16)
            for q in range(slabs):
                scat_v[q * rhs : (q + 1) * rhs, cols] = jnp.where(
                    high == jnp.full((), q, BF16), value, zero
                )
        done = nt(scat_v[...], hot_v[...])
        for q in range(slabs):
            out_v[slot, :, q * leaf : (q + 1) * leaf] = done[q * rhs : (q + 1) * rhs]
        copy = pltpu.make_async_copy(out_v.at[slot], target, out_sem.at[slot])
        copy.start()
        return copy

    def wait_sends(a):
        for k in range(len(line)):
            r1_copy(a, k).wait_send()
        for k in range(len(plane)):
            r2_copy(a, k).wait_send()
        for n in range(len(sides)):
            raw_copy(a, n).wait_send()
        for n in range(4):
            halo_copy(a, n).wait_send()

    send_up(0, msg)
    send_halos(0)

    eye = placed(rank, rank, 0).astype(BF16)
    square = jnp.zeros((rank, rank), F32)
    for l in range(leaves):
        turned = nt(eye, lt_v[l]).astype(BF16)
        qt = halves(nn(turned, basis_v[l]))
        qt_v[l] = qt
        square = square + nt(qt[0:rank], qt[0:rank])
    c_dc.wait()
    c_bc.wait()
    c_tc.wait()
    e2 = parts_of(full(square, *e1) + placed(rank, 4 * rank, 2 * rank))
    picks = [placed(LINKS * rank, rank, -k * rank).astype(BF16) for k in range(LINKS)]
    sides_in = [nn(dc_v[0], pick) for pick in picks]
    blocks_in = [nt(nn(bc_v[0], pick).astype(BF16), own_dt) for pick in picks]
    tops_in = [
        fine(nt, nt(nn(tc_v[0], pick).astype(BF16), own_bt), own_dt) for pick in picks
    ]
    mixed = full(jnp.concatenate(sides_in + blocks_in + tops_in, axis=0), *e2)
    mix_v[...] = jnp.zeros_like(mix_v)
    for n in range(3 * LINKS):
        base = n * 2 * rank + (0 if LINKS <= n < 2 * LINKS else rank)
        for half, value in enumerate(parts_of(mixed[n * rank : (n + 1) * rank])):
            mix_v[half, base : base + rank, :] = value


    send_across(0)

    c_tiles.wait()
    c_lc.wait()
    wait_halos(0)
    near_and_leaf(0)
    local = jnp.zeros((rhs, rank), F32)
    for l in range(leaves):
        local = local + nt(near_v[l].astype(BF16), qt_v[l, 0:rank])
    partial = full(local, *e1) + side_part(0)

    wait_across(0)
    msg = partial + far_part(0)
    send_up(1, msg)

    field = field_of(msg)
    for l in range(leaves):
        value = near_v[l] + twice_rows(nn(field, qt_v[l]))
        near_v[l] = value
        value = value.astype(BF16)
        vw[1][NEAR_REACH + l] = value
        mw[1][LINK_REACH + l] = moments_of(value, l)
    send_halos(1)
    send_across(1)
    c_smoothed = scatter(smoothed, 0)
    wait_halos(1)
    near_and_leaf(1)
    partial = side_part(1)
    wait_sends(0)
    wait_sends(1)
    wait_across(1)
    msg = partial + far_part(1)
    field = field_of(msg)
    for l in range(leaves):
        near_v[l] = near_v[l] + twice_rows(nn(field, qt_v[l]))
    c_twice = scatter(twice, 1)
    c_smoothed.wait()
    c_twice.wait()


def publish(first, second, smoothed, twice, held, sems):
    pairs = ((first, smoothed), (second, twice))
    loads = [
        pltpu.make_async_copy(src, held.at[n], sems.at[n])
        for n, (src, dst) in enumerate(pairs)
    ]
    stores = [
        pltpu.make_async_copy(held.at[n], dst, sems.at[2 + n])
        for n, (src, dst) in enumerate(pairs)
    ]
    for copy in loads:
        copy.start()
    for load, store in zip(loads, stores):
        load.wait()
        store.start()
    for copy in stores:
        copy.wait()


def solution(mesh):
    sizes = mesh.shape["gx"], mesh.shape["gy"], mesh.shape["gz"]
    n_gx, n_gy, n_gz = sizes

    def shards(
        signal,
        order,
        near_tiles,
        near_list,
        leaf_basis,
        leaf_transfer,
        leaf_coupling,
        leaf_links,
        device_transfer,
        device_coupling,
        device_links,
        block_transfer,
        block_coupling,
        block_links,
        top_coupling,
        top_links,
    ):
        rhs, points = signal.shape
        leaves, rank, leaf = leaf_basis.shape
        n_blocks = n_gx * n_gy
        vmem, far = pltpu.VMEM, pl.BlockSpec(memory_space=pl.ANY)
        smem = pl.BlockSpec(memory_space=pltpu.SMEM)
        wide = 2 * rank
        dma = pltpu.SemaphoreType.DMA
        scratch = [
            vmem((rhs, points), F32),
            vmem((1, points), jnp.int32),
            vmem(near_tiles.shape, BF16),
            vmem(leaf_basis.shape, BF16),
            vmem(leaf_transfer.shape, BF16),
            vmem(leaf_coupling.shape, BF16),
            vmem(device_transfer.shape, BF16),
            vmem(device_coupling.shape, BF16),
            vmem(block_transfer.shape, BF16),
            vmem(block_coupling.shape, BF16),
            vmem(top_coupling.shape, BF16),
            vmem((leaf, points), BF16),
            vmem((rhs * points // leaf, points), BF16),
            vmem((leaves + 2 * NEAR_REACH, rhs, leaf), BF16),
            vmem((leaves + 2 * NEAR_REACH, rhs, leaf), BF16),
            vmem((leaves + 2 * LINK_REACH, rhs, wide), BF16),
            vmem((leaves + 2 * LINK_REACH, rhs, wide), BF16),
            vmem((2 * DEVICE_REACH + 1, rhs, wide), F32),
            vmem((2 * DEVICE_REACH + 1, rhs, wide), F32),
            vmem((2, rhs, wide), BF16),
            vmem((2, n_gz, rhs, wide), BF16),
            vmem((n_blocks, rhs, wide), BF16),
            vmem((n_blocks, rhs, wide), BF16),
            vmem((leaves, rhs, leaf), F32),
            vmem((2 * leaves * rhs, LINKS * rank), BF16),
            vmem((leaves, 2 * rank, leaf), BF16),
            vmem((2, 3 * LINKS * wide, 4 * rank), BF16),
            vmem((2, rhs, points), F32),
            dma((11,)),
            dma((2,)),
            dma((2, 4)),
            dma((2, 4)),
            dma((2, 6)),
            dma((2, 6)),
            dma((2, n_gz)),
            dma((2, n_gz)),
            dma((2, n_blocks)),
            dma((2, n_blocks)),
        ]
        out = jax.ShapeDtypeStruct((rhs, points), F32)
        results = pl.pallas_call(
            functools.partial(kernel, n_gx, n_gy, n_gz),
            out_shape=(out, out),
            in_specs=[smem] * 5 + [far] * 11,
            out_specs=(far,) * 2,
            scratch_shapes=scratch,
            compiler_params=pltpu.CompilerParams(
                collective_id=0, has_side_effects=True, vmem_limit_bytes=60 * 1024 * 1024
            ),
        )(
            near_list.T,
            leaf_links.T,
            device_links,
            block_links,
            top_links,
            signal,
            order.reshape(1, points),
            near_tiles,
            leaf_basis,
            leaf_transfer,
            leaf_coupling,
            device_transfer,
            device_coupling,
            block_transfer,
            block_coupling,
            top_coupling,
        )
        return pl.pallas_call(
            publish,
            out_shape=(out, out),
            in_specs=[far] * 2,
            out_specs=(far,) * 2,
            scratch_shapes=[vmem((2, rhs, points), F32), dma((4,))],
        )(*results)

    every = ("gx", "gy", "gz")
    in_specs = (
        P(None, every),
        P(every),
        P(every, None, None, None),
        P(every, None),
        P(every, None, None),
        P(every, None, None),
        P(every, None, None),
        P(every, None),
        P(every, None, None),
        P(every, None, None),
        P(every, None),
        P(("gx", "gy"), None, None),
        P(("gx", "gy"), None, None),
        P(("gx", "gy"), None),
        P("gx", None, None),
        P("gx", None),
    )
    out_specs = (P(None, every), P(None, every))
    return jax.shard_map(
        shards, mesh=mesh, in_specs=in_specs, out_specs=out_specs, check_vma=False
    )
```

```python
import functools

import jax
import jax.numpy as jnp
from jax import lax
from jax.experimental import pallas as pl
from jax.experimental.pallas import tpu as pltpu
from jax.sharding import PartitionSpec as P

MESH = pl.DeviceIdType.MESH
NEAR_REACH = 2
LINK_REACH = 4
DEVICE_REACH = 3
LINKS = 3
F32 = jnp.float32
BF16 = jnp.bfloat16


def nn(a, b):
    return lax.dot_general(a, b, (((1,), (0,)), ((), ())), preferred_element_type=F32)


def nt(a, b):
    return lax.dot_general(a, b, (((1,), (1,)), ((), ())), preferred_element_type=F32)


def within(index, ref):
    return jnp.minimum(jnp.maximum(index, 0), ref.shape[0] - 1)


def halves(x):
    top = x.astype(BF16)
    return jnp.concatenate([top, (x - top.astype(F32)).astype(BF16)], axis=0)


def fine(product, x, weights):
    both = product(halves(x), weights)
    return both[: x.shape[0]] + both[x.shape[0] :]


def parts_of(x):
    top = x.astype(BF16)
    return top, (x - top.astype(F32)).astype(BF16)


def full(x, tops, rests):
    both = nn(halves(x), tops)
    return both[: x.shape[0]] + both[x.shape[0] :] + nn(x.astype(BF16), rests)


def placed(rows, cols, offset):
    i = lax.broadcasted_iota(jnp.int32, (rows, cols), 0)
    j = lax.broadcasted_iota(jnp.int32, (rows, cols), 1)
    return jnp.where(j == i + offset, 1.0, 0.0).astype(F32)


def kernel(
    n_gx,
    n_gy,
    n_gz,
    near_list_in,
    leaf_links_in,
    device_links_in,
    block_links_in,
    top_links_in,
    signal,
    order,
    near_tiles,
    leaf_basis,
    leaf_transfer,
    leaf_coupling,
    device_transfer,
    device_coupling,
    block_transfer,
    block_coupling,
    top_coupling,
    smoothed,
    twice,
    near_list,
    leaf_links,
    device_links,
    block_links,
    top_links,
    sig_v,
    ord_v,
    tiles_v,
    basis_v,
    lt_v,
    lc_v,
    dt_v,
    dc_v,
    bt_v,
    bc_v,
    tc_v,
    hot_v,
    scat_v,
    vw_0,
    vw_1,
    mw_0,
    mw_1,
    raw_0,
    raw_1,
    r1_src,
    r1_buf,
    r2_0,
    r2_1,
    near_v,
    coup_v,
    qt_v,
    mix_v,
    out_v,
    local_sem,
    out_sem,
    halo_send,
    halo_recv,
    raw_send,
    raw_recv,
    r1_send,
    r1_recv,
    r2_send,
    r2_recv,
):
    rhs, points = sig_v.shape
    leaves, rank, leaf = basis_v.shape
    slabs = points // leaf
    shift = leaf.bit_length() - 1
    assert 1 << shift == leaf
    n_blocks = n_gx * n_gy
    n_devices = n_blocks * n_gz
    gx, gy, gz = lax.axis_index("gx"), lax.axis_index("gy"), lax.axis_index("gz")
    block = gx * n_gy + gy
    device = block * n_gz + gz
    first_leaf = device * leaves

    def wrapped(index, size):
        index = jnp.where(index >= size, index - size, index)
        return jnp.where(index < 0, index + size, index)

    def mesh_id(shift):
        z = gz + shift
        carry = (z >= n_gz).astype(jnp.int32) - (z < 0).astype(jnp.int32)
        y = gy + carry
        carry = (y >= n_gy).astype(jnp.int32) - (y < 0).astype(jnp.int32)
        return {
            "gx": wrapped(gx + carry, n_gx),
            "gy": wrapped(y, n_gy),
            "gz": wrapped(z, n_gz),
        }

    def far_first(size):
        return sorted(range(size), key=lambda step: -min(step, size - step))

    plane = [(x, y) for x in far_first(n_gx) for y in far_first(n_gy) if x or y]

    def plane_id(k):
        x, y = plane[k]
        return {"gx": wrapped(gx + x, n_gx), "gy": wrapped(gy + y, n_gy), "gz": gz}

    line = [step for step in far_first(n_gz) if step]

    def line_id(k):
        return {"gx": gx, "gy": gy, "gz": wrapped(gz + line[k], n_gz)}

    sides = (-3, -2, -1, 1, 2, 3)
    vw, mw, raw_v, r2_buf = (vw_0, vw_1), (mw_0, mw_1), (raw_0, raw_1), (r2_0, r2_1)

    def load(src, dst, slot):
        copy = pltpu.make_async_copy(src, dst, local_sem.at[slot])
        copy.start()
        return copy

    c_order = load(order, ord_v, 0)
    c_signal = load(signal, sig_v, 1)
    c_dt = load(device_transfer, dt_v, 2)
    c_bt = load(block_transfer, bt_v, 3)
    c_basis = load(leaf_basis, basis_v, 4)
    c_lt = load(leaf_transfer, lt_v, 5)
    c_dc = load(device_coupling, dc_v, 6)
    c_bc = load(block_coupling, bc_v, 7)
    c_tc = load(top_coupling, tc_v, 8)
    c_tiles = load(near_tiles, tiles_v, 9)
    c_lc = load(leaf_coupling, lc_v, 10)
    c_lists = [
        load(near_list_in, near_list, 11),
        load(leaf_links_in, leaf_links, 12),
        load(device_links_in, device_links, 13),
        load(block_links_in, block_links, 14),
        load(top_links_in, top_links, 15),
    ]

    barrier = pltpu.get_barrier_semaphore()

    peers = [plane_id(k) for k in range(len(plane))]
    peers = peers + [line_id(k) for k in range(len(line))] + [mesh_id(s) for s in sides]
    for peer in peers:
        pl.semaphore_signal(barrier, inc=1, device_id=peer, device_id_type=MESH)

    mix_v[...] = jnp.zeros_like(mix_v)

    c_order.wait()
    c_signal.wait()
    sig_rows = jnp.concatenate(
        [sig_v[:, q * leaf : (q + 1) * leaf].astype(BF16) for q in range(slabs)], axis=0
    )
    def narrow(x):
        return x.astype(F32).astype(BF16)

    one, zero = jnp.ones((), BF16), jnp.zeros((), BF16)
    lane_rows = narrow(lax.broadcasted_iota(jnp.int32, (leaf, leaf), 0))
    upper_lanes = lax.broadcasted_iota(jnp.int32, (rhs, 2 * rank), 1) >= rank

    def twofold(x):
        return jnp.concatenate([x, x], axis=0)

    def moments_of(value, l):
        both = nt(value, twofold(basis_v[l]))
        top = both.astype(BF16).astype(F32)
        return jnp.where(upper_lanes, both - top, top).astype(BF16)

    for j in range(leaves):
        cols = slice(j * leaf, (j + 1) * leaf)
        spot = ord_v[:, cols]
        low = spot & (leaf - 1)
        high = lax.shift_right_logical(spot, shift)
        hot = jnp.where(lane_rows == narrow(low), one, zero)
        hot_v[:, cols] = hot
        picked = nn(sig_rows, hot)
        value = jnp.zeros((rhs, leaf), F32)
        for q in range(slabs):
            value = value + jnp.where(high == q, picked[q * rhs : (q + 1) * rhs], 0.0)
        value = value.astype(BF16)
        vw[0][NEAR_REACH + j] = value
    c_basis.wait()
    c_lt.wait()
    moments = [moments_of(vw[0][NEAR_REACH + j], j) for j in range(leaves)]
    for j in range(leaves):
        mw[0][LINK_REACH + j] = moments[j]
    weights = [twofold(lt_v[j]) for j in range(leaves)]
    own = nn(jnp.concatenate(moments, axis=1), jnp.concatenate(weights, axis=0))

    c_dt.wait()
    c_bt.wait()
    own_dt = dt_v[0]
    own_bt = bt_v[0]
    up = placed(rank, 4 * rank, 0) + nn(own_bt, placed(rank, 4 * rank, rank).astype(BF16))
    e1 = parts_of(nn(own_dt, up.astype(BF16)) + placed(rank, 4 * rank, 3 * rank))

    msg = full(own, *e1)

    pl.semaphore_wait(barrier, len(peers))

    def r1_copy(a, k):
        return pltpu.make_async_remote_copy(
            src_ref=r1_src.at[a],
            dst_ref=r1_buf.at[a, k],
            send_sem=r1_send.at[a],
            recv_sem=r1_recv.at[a],
            device_id=line_id(k),
            device_id_type=MESH,
        )

    def r2_copy(a, k):
        return pltpu.make_async_remote_copy(
            src_ref=r2_buf[a].at[block],
            dst_ref=r2_buf[a].at[block],
            send_sem=r2_send.at[a],
            recv_sem=r2_recv.at[a],
            device_id=plane_id(k),
            device_id_type=MESH,
        )

    def raw_copy(a, n):
        s = sides[n]
        return pltpu.make_async_remote_copy(
            src_ref=raw_v[a].at[DEVICE_REACH],
            dst_ref=raw_v[a].at[DEVICE_REACH - s],
            send_sem=raw_send.at[a],
            recv_sem=raw_recv.at[a],
            device_id=mesh_id(s),
            device_id_type=MESH,
        )

    def halo_copy(a, n):
        ref, reach = (vw, NEAR_REACH) if n < 2 else (mw, LINK_REACH)
        if n % 2 == 0:
            src, dst, s = leaves, 0, 1
        else:
            src, dst, s = reach, reach + leaves, -1
        return pltpu.make_async_remote_copy(
            src_ref=ref[a].at[pl.ds(src, reach)],
            dst_ref=ref[a].at[pl.ds(dst, reach)],
            send_sem=halo_send.at[a],
            recv_sem=halo_recv.at[a],
            device_id=mesh_id(s),
            device_id_type=MESH,
        )

    def group(ref, count, sem):
        ref = ref.at[pl.ds(0, count)]
        return pltpu.make_async_copy(ref, ref, sem)

    def r1_all(a, sem):
        return group(r1_buf.at[a], len(line), sem.at[a])

    def r2_all(a, sem):
        return group(r2_buf[a], len(plane), sem.at[a])

    def raw_all(a, sem):
        return group(raw_v[a], len(sides), sem.at[a])

    def halo_all(a, sem):
        return group(vw[a], 2 * (NEAR_REACH + NEAR_REACH), sem.at[a])

    def send_up(a, message):
        r1_src[a] = message[:, 0 : 2 * rank].astype(BF16)
        raw_v[a][DEVICE_REACH] = message[:, 2 * rank : 4 * rank]

        for k in range(len(line)):
            r1_copy(a, k).start()
        for n in range(len(sides)):
            raw_copy(a, n).start()

    def send_across(a):
        r1_all(a, r1_recv).wait()
        total = r1_src[a].astype(F32)
        for k in range(len(line)):
            total = total + r1_buf[a, k].astype(F32)
        r2_buf[a][block] = total.astype(BF16)
        for k in range(len(plane)):
            r2_copy(a, k).start()

    def wait_across(a):
        r2_all(a, r2_recv).wait()

    def far_part(a):
        parts = [r2_buf[a][block_links[0, k]].astype(BF16) for k in range(LINKS)]
        for k in range(LINKS):
            total = jnp.zeros((rhs, 2 * rank), F32)
            for i in range(n_gy):
                total = total + r2_buf[a][top_links[0, k] * n_gy + i].astype(F32)
            parts.append(total.astype(BF16))
        rows = jnp.concatenate(parts, axis=1)
        start = LINKS * 2 * rank
        return nn(rows, mix_v[0, start:]) + nn(rows, mix_v[1, start:])

    def side_part(a):
        raw_all(a, raw_recv).wait()
        parts = [
            raw_v[a][within(device_links[0, k] - device + DEVICE_REACH, raw_v[a])]
            for k in range(LINKS)
        ]
        end = LINKS * 2 * rank
        return full(jnp.concatenate(parts, axis=1), mix_v[0, :end], mix_v[1, :end])

    def field_of(message):
        field = message[:, 2 * rank : 3 * rank]
        return halves(jnp.concatenate([field, field], axis=1))

    def twice_rows(both):
        return both[0:rhs] + both[rhs:]

    def send_halos(a):
        for n in range(4):
            halo_copy(a, n).start()

    def wait_halos(a):
        halo_all(a, halo_recv).wait()

    def near_and_leaf(a):
        diagonal = lax.broadcasted_iota(jnp.int32, (rhs, LINKS * rank), 1) // rank
        for l in range(leaves):
            total = nn(vw[a][NEAR_REACH + l], tiles_v[l, 0])
            for k in range(1, near_list.shape[0]):
                spot = within(near_list[k, l] - first_leaf + NEAR_REACH, vw[a])
                total = total + nn(vw[a][spot], tiles_v[l, k])
            near_v[l] = total
            stacked = jnp.concatenate(
                [
                    mw[a][within(leaf_links[k, l] - first_leaf + LINK_REACH, mw[a])]
                    for k in range(LINKS)
                ],
                axis=0,
            )
            wide = nn(stacked, twofold(lc_v[l]))
            kept = wide[0:rhs]
            for k in range(1, LINKS):
                kept = jnp.where(diagonal == k, wide[k * rhs : (k + 1) * rhs], kept)
            coup_v[l * 2 * rhs : (l + 1) * 2 * rhs, :] = halves(kept)
        fold = placed(LINKS * rank, rank, 0)
        for k in range(1, LINKS):
            fold = fold + placed(LINKS * rank, rank, -k * rank)
        field = nn(coup_v[...], fold.astype(BF16))
        for l in range(leaves):
            base = l * 2 * rhs
            whole = field[base : base + rhs] + field[base + rhs : base + 2 * rhs]
            near_v[l] = near_v[l] + fine(nn, whole, basis_v[l])

    def scatter(target, slot):
        for j in range(leaves):
            cols = slice(j * leaf, (j + 1) * leaf)
            high = narrow(lax.shift_right_logical(ord_v[:, cols], shift))
            value = near_v[j].astype(BF16)
            for q in range(slabs):
                scat_v[q * rhs : (q + 1) * rhs, cols] = jnp.where(
                    high == jnp.full((), q, BF16), value, zero
                )
        done = nt(scat_v[...], hot_v[...])
        for q in range(slabs):
            out_v[slot, :, q * leaf : (q + 1) * leaf] = done[q * rhs : (q + 1) * rhs]
        copy = pltpu.make_async_copy(out_v.at[slot], target, out_sem.at[slot])
        copy.start()
        return copy

    def wait_sends(a):
        r1_all(a, r1_send).wait()
        r2_all(a, r2_send).wait()
        raw_all(a, raw_send).wait()
        halo_all(a, halo_send).wait()

    send_up(0, msg)
    send_halos(0)

    c_dc.wait()
    c_bc.wait()
    c_tc.wait()
    picks = [placed(LINKS * rank, rank, -k * rank).astype(BF16) for k in range(LINKS)]
    sides_in = [nn(dc_v[0], pick) for pick in picks]
    blocks_in = [nt(nn(bc_v[0], pick).astype(BF16), own_dt) for pick in picks]
    tops_in = [
        fine(nt, nt(nn(tc_v[0], pick).astype(BF16), own_bt), own_dt) for pick in picks
    ]
    eye = placed(rank, rank, 0).astype(BF16)
    square = jnp.zeros((rank, rank), F32)
    for l in range(leaves):
        turned = nt(eye, lt_v[l]).astype(BF16)
        qt = halves(nn(turned, basis_v[l]))
        qt_v[l] = qt
        square = square + nt(qt[0:rank], qt[0:rank])
    e2 = parts_of(full(square, *e1) + placed(rank, 4 * rank, 2 * rank))
    mixed = full(jnp.concatenate(sides_in + blocks_in + tops_in, axis=0), *e2)
    for n in range(3 * LINKS):
        base = n * 2 * rank + (0 if LINKS <= n < 2 * LINKS else rank)
        for half, value in enumerate(parts_of(mixed[n * rank : (n + 1) * rank])):
            mix_v[half, base : base + rank, :] = value


    send_across(0)

    for copy in c_lists:
        copy.wait()
    c_tiles.wait()
    c_lc.wait()
    wait_halos(0)
    near_and_leaf(0)
    local = jnp.zeros((rhs, rank), F32)
    for l in range(leaves):
        local = local + nt(near_v[l].astype(BF16), qt_v[l, 0:rank])
    partial = full(local, *e1) + side_part(0)

    wait_across(0)
    msg = partial + far_part(0)
    send_up(1, msg)

    field = field_of(msg)
    for l in range(leaves):
        value = near_v[l] + twice_rows(nn(field, qt_v[l]))
        near_v[l] = value
        value = value.astype(BF16)
        vw[1][NEAR_REACH + l] = value
        mw[1][LINK_REACH + l] = moments_of(value, l)
    send_halos(1)
    send_across(1)
    c_smoothed = scatter(smoothed, 0)
    wait_halos(1)
    near_and_leaf(1)
    partial = side_part(1)
    wait_sends(0)
    wait_sends(1)
    wait_across(1)
    msg = partial + far_part(1)
    field = field_of(msg)
    for l in range(leaves):
        near_v[l] = near_v[l] + twice_rows(nn(field, qt_v[l]))
    c_twice = scatter(twice, 1)
    c_smoothed.wait()
    c_twice.wait()


def publish(first, second, smoothed, twice, held, sems):
    pairs = ((first, smoothed), (second, twice))
    loads = [
        pltpu.make_async_copy(src, held.at[n], sems.at[n])
        for n, (src, dst) in enumerate(pairs)
    ]
    stores = [
        pltpu.make_async_copy(held.at[n], dst, sems.at[2 + n])
        for n, (src, dst) in enumerate(pairs)
    ]
    for copy in loads:
        copy.start()
    for load, store in zip(loads, stores):
        load.wait()
        store.start()
    for copy in stores:
        copy.wait()


def solution(mesh):
    sizes = mesh.shape["gx"], mesh.shape["gy"], mesh.shape["gz"]
    n_gx, n_gy, n_gz = sizes

    def shards(
        signal,
        order,
        near_tiles,
        near_list,
        leaf_basis,
        leaf_transfer,
        leaf_coupling,
        leaf_links,
        device_transfer,
        device_coupling,
        device_links,
        block_transfer,
        block_coupling,
        block_links,
        top_coupling,
        top_links,
    ):
        rhs, points = signal.shape
        leaves, rank, leaf = leaf_basis.shape
        n_blocks = n_gx * n_gy
        vmem, far = pltpu.VMEM, pl.BlockSpec(memory_space=pl.ANY)
        wide = 2 * rank
        dma = pltpu.SemaphoreType.DMA
        lists = (near_list.T, leaf_links.T, device_links, block_links, top_links)
        scratch = [pltpu.SMEM(x.shape, jnp.int32) for x in lists] + [
            vmem((rhs, points), F32),
            vmem((1, points), jnp.int32),
            vmem(near_tiles.shape, BF16),
            vmem(leaf_basis.shape, BF16),
            vmem(leaf_transfer.shape, BF16),
            vmem(leaf_coupling.shape, BF16),
            vmem(device_transfer.shape, BF16),
            vmem(device_coupling.shape, BF16),
            vmem(block_transfer.shape, BF16),
            vmem(block_coupling.shape, BF16),
            vmem(top_coupling.shape, BF16),
            vmem((leaf, points), BF16),
            vmem((rhs * points // leaf, points), BF16),
            vmem((leaves + 2 * NEAR_REACH, rhs, leaf), BF16),
            vmem((leaves + 2 * NEAR_REACH, rhs, leaf), BF16),
            vmem((leaves + 2 * LINK_REACH, rhs, wide), BF16),
            vmem((leaves + 2 * LINK_REACH, rhs, wide), BF16),
            vmem((2 * DEVICE_REACH + 1, rhs, wide), F32),
            vmem((2 * DEVICE_REACH + 1, rhs, wide), F32),
            vmem((2, rhs, wide), BF16),
            vmem((2, n_gz, rhs, wide), BF16),
            vmem((n_blocks, rhs, wide), BF16),
            vmem((n_blocks, rhs, wide), BF16),
            vmem((leaves, rhs, leaf), F32),
            vmem((2 * leaves * rhs, LINKS * rank), BF16),
            vmem((leaves, 2 * rank, leaf), BF16),
            vmem((2, 3 * LINKS * wide, 4 * rank), BF16),
            vmem((2, rhs, points), F32),
            dma((16,)),
            dma((2,)),
            dma((2,)),
            dma((2,)),
            dma((2,)),
            dma((2,)),
            dma((2,)),
            dma((2,)),
            dma((2,)),
            dma((2,)),
        ]
        out = jax.ShapeDtypeStruct((rhs, points), F32)
        results = pl.pallas_call(
            functools.partial(kernel, n_gx, n_gy, n_gz),
            out_shape=(out, out),
            in_specs=[far] * 16,
            out_specs=(far,) * 2,
            scratch_shapes=scratch,
            compiler_params=pltpu.CompilerParams(
                collective_id=0, has_side_effects=True, vmem_limit_bytes=60 * 1024 * 1024
            ),
        )(
            *lists,
            signal,
            order.reshape(1, points),
            near_tiles,
            leaf_basis,
            leaf_transfer,
            leaf_coupling,
            device_transfer,
            device_coupling,
            block_transfer,
            block_coupling,
            top_coupling,
        )
        return pl.pallas_call(
            publish,
            out_shape=(out, out),
            in_specs=[far] * 2,
            out_specs=(far,) * 2,
            scratch_shapes=[vmem((2, rhs, points), F32), dma((4,))],
        )(*results)

    every = ("gx", "gy", "gz")
    in_specs = (
        P(None, every),
        P(every),
        P(every, None, None, None),
        P(every, None),
        P(every, None, None),
        P(every, None, None),
        P(every, None, None),
        P(every, None),
        P(every, None, None),
        P(every, None, None),
        P(every, None),
        P(("gx", "gy"), None, None),
        P(("gx", "gy"), None, None),
        P(("gx", "gy"), None),
        P("gx", None, None),
        P("gx", None),
    )
    out_specs = (P(None, every), P(None, every))
    return jax.shard_map(
        shards, mesh=mesh, in_specs=in_specs, out_specs=out_specs, check_vma=False
    )
```
